32 devices in a mesh: shard: 4 (over z), replica: 8 (over y, x, core).
Axes of the slice: x: 2, y: 2, z: 4, core: 2. Of those that a mesh axis runs over, the one named last changes fastest.
Arguments:
- atom_feats: bfloat16 [2048, 9, 128], P(('shard', 'replica')), may hold values from -6 to 6
- cotangent: bfloat16 [2048, 9, 128], P(('shard', 'replica')), may hold values from -6 to 6
- frames: bfloat16 [9, 9, 8192], P(None, None, ('shard', 'replica')), may hold values from -2 to 2
- radial: bfloat16 [8192, 128], P(('shard', 'replica')), may hold values from 0.19921875 to 2
- edge_source: int32 [8192], P(('shard', 'replica')), may hold values from 0 to 63
- edge_target: int32 [8192], P(('shard', 'replica')), may hold values from 0 to 63
- edge_valid: int32 [8192], P(('shard', 'replica')), may hold values 0 or 1
- atom_types: int32 [2048], P(('shard', 'replica')), may hold values from 0 to 99
- dataset: int32 [32], P(('shard', 'replica')), may hold values from 0 to 4
- type_table: float32 [100, 128], replicated, may hold values from -6 to 6
- dataset_table: float32 [5, 128], replicated, may hold values from -6 to 6
- router_weight: float32 [128, 28], replicated, may hold values from -1.5 to 1.5
- experts: bfloat16 [28, 384, 384], P(None, 'shard'), may hold values from -3 to 3
Outputs:
- updated: bfloat16 [2048, 9, 128], P(('shard', 'replica'))
- feats_grad: float32 [2048, 9, 128], P(('shard', 'replica'))
- expert_grad: float32 [28, 384, 384], P(None, 'shard')
The draws below stay inside these ranges and needn't reach their ends.
Inputs may be any that keep to these rules, and one draw needn't show every extreme that they name: `edge_source`: indices of atoms within the edge's own system. `edge_target`: indices of atoms within the edge's own system.
All inputs are finite; a program needn't handle non-finite values. No bound on the sum of `edge_valid` on one device may be relied on, other than what follows from the above.
Results may differ from the reference program's by a relative error of at most 0.011.
Values may be sent and summed in bfloat16 or wider, within the bound.
A program may use at most 64 MiB of HBM per device.

```python
import math
import jax
import jax.numpy as jnp
import numpy as np
from jax import lax

C = 128
LMAX = 2
EXPERTS = 28
TYPES = 100
DATASETS = 5
A_DEV = 64
E_DEV = 256
COEFS = 9
SYSTEMS = 32
ATOMS = 2048
EDGES = 8192
N_SHARD = 4
N_REPLICA = 8


def with_ends(array, own_key, least, top_value):
    index_at = [jax.random.randint(jax.random.fold_in(own_key, axis), (), 0, length) for axis, length in enumerate(array.shape)]
    longest = array.shape.index(max(array.shape))
    beside = index_at[:longest] + [(index_at[longest] + 1) % array.shape[longest]] + index_at[longest + 1:]
    return array.at[tuple(index_at)].set(least).at[tuple(beside)].set(top_value)


def shard_levels(rng, extent, pieces, smallest, largest):
    gain = 1.0
    for dim, shards_of in pieces:
        steps = jax.random.uniform(jax.random.fold_in(jax.random.fold_in(rng, 6), dim), (shards_of,), jnp.float32, smallest / len(pieces), largest / len(pieces))
        gain = gain * jnp.repeat(jnp.exp(steps), extent[dim] // shards_of).reshape((-1,) + (1,) * (len(extent) - 1 - dim))
    return gain


def rank_bounds(amount, skew):
    loads = [(1 << 20) // math.isqrt(grade ** skew) + 1 for grade in range(1, amount + 1)]
    deviation = 1 + sum(loads) // (1 << 30)
    return np.cumsum(np.array([max(1, weight // deviation) for weight in loads]))


def skewed_ids(key, extent, number_of, lean):
    grid = rank_bounds(number_of, lean)
    ticket = jax.random.randint(jax.random.fold_in(key, 1), extent, 0, int(grid[number_of - 1]))
    standing = jnp.searchsorted(jnp.asarray(grid, jnp.int32), ticket, side="right")
    return jax.random.permutation(jax.random.fold_in(key, 2), number_of)[standing].astype(jnp.int32)


def scatter_about(key, extent, deviation, most, shards=(), kind=jnp.bfloat16):
    level = shard_levels(key, extent, shards, -0.22, 0.18) if shards else 1.0
    array = jax.random.normal(key, extent, jnp.float32) * deviation * level
    return jnp.minimum(jnp.maximum(array, -most), most).astype(kind)


def setup_inputs(seed: int = 0) -> dict:
    keys = jax.random.split(jax.random.key(seed), 14)
    return {
        "atom_feats": scatter_about(keys[0], (ATOMS, COEFS, C), 1.0, 6.0, ((0, 32),)),
        "cotangent": scatter_about(keys[1], (ATOMS, COEFS, C), 1.0, 6.0, ((0, 32),)),
        "frames": scatter_about(keys[2], (COEFS, COEFS, EDGES), COEFS ** -0.5, 2.0, ((2, 32),)),
        "radial": jnp.clip(jnp.exp(math.log(2.0) - 2.306499 * jax.random.uniform(keys[3], (EDGES, C), jnp.float32) ** shard_levels(keys[3], (EDGES, C), ((0, 32),), -0.2, 0.2)), 0.19921875, 2.0).astype(jnp.bfloat16),
        "edge_source": with_ends(jax.random.randint(keys[4], (EDGES,), 0, A_DEV), jax.random.fold_in(keys[4], 1), 0, A_DEV - 1).astype(jnp.int32),
        "edge_target": with_ends(jax.random.randint(keys[5], (EDGES,), 0, A_DEV), jax.random.fold_in(keys[5], 1), 0, A_DEV - 1).astype(jnp.int32),
        "edge_valid": with_ends((jax.random.randint(keys[6], (EDGES,), 0, 8) < 7).astype(jnp.int32), jax.random.fold_in(keys[6], 1), 0, 1),
        "atom_types": with_ends(skewed_ids(keys[7], (ATOMS,), TYPES, 2), jax.random.fold_in(keys[7], 3), 0, TYPES - 1).astype(jnp.int32),
        "dataset": with_ends(jax.random.randint(keys[8], (SYSTEMS,), 0, DATASETS), jax.random.fold_in(keys[8], 1), 0, DATASETS - 1).astype(jnp.int32),
        "type_table": scatter_about(keys[9], (TYPES, C), 1.0, 6.0, (), jnp.float32),
        "dataset_table": scatter_about(keys[10], (DATASETS, C), 1.0, 6.0, (), jnp.float32),
        "router_weight": scatter_about(keys[11], (C, EXPERTS), (C // 8) ** -0.5, 1.5, (), jnp.float32),
        "experts": scatter_about(keys[12], (EXPERTS, (LMAX + 1) * C, (LMAX + 1) * C), (4.0 / ((LMAX + 1) * C) ** 0.5), 3.0, ((1, 4),)),
    }


def system_mix(type_rows, dataset_one, type_table, dataset_table, router_weight):
    table_size = type_table.shape[0]
    onehot = (type_rows[:, None] == jnp.arange(table_size, dtype=jnp.int32)[None, :]).astype(jnp.float32)
    counts = lax.optimization_barrier(jnp.sum(onehot, axis=0))
    embed = jnp.dot(counts, type_table, precision=lax.Precision.HIGHEST) / type_rows.shape[0]
    pick = (dataset_one[:, None] == jnp.arange(dataset_table.shape[0], dtype=jnp.int32)[None, :]).astype(jnp.float32)
    embed = embed + jnp.dot(pick, dataset_table, precision=lax.Precision.HIGHEST)[0]
    soft = jax.nn.softplus(jnp.dot(embed, router_weight, precision=lax.Precision.HIGHEST))
    return soft / jnp.sum(soft)

def edge_layer(feats32, merged32, frames, radial, source, target, valid):
    atom_count, components, channels = feats32.shape
    edge_count = source.shape[0]
    top_degree = math.isqrt(components) - 1
    feats = feats32.astype(jnp.bfloat16)
    merged = merged32.astype(jnp.bfloat16)
    gathered = jnp.take(feats, source, axis=0)
    rotated = jnp.einsum('ije,ejc->eic', frames.astype(jnp.float32), gathered.astype(jnp.float32)).astype(jnp.bfloat16)
    zero_rows = [degree * degree + degree for degree in range(top_degree + 1)]
    zero_band = jnp.concatenate([rotated[:, row:row + 1, :] for row in zero_rows], axis=1).reshape(edge_count, -1)
    mixed_band = jnp.dot(zero_band, merged, preferred_element_type=jnp.float32).reshape(edge_count, top_degree + 1, channels)
    columns = []
    for column in range(components):
        if column in zero_rows:
            columns.append(mixed_band[:, zero_rows.index(column), :])
        else:
            columns.append(rotated[:, column, :].astype(jnp.float32))
    combined = jnp.stack(columns, axis=1)
    message = (combined * radial.astype(jnp.float32)[:, None, :]).astype(jnp.bfloat16)
    unrotated = jnp.einsum('jie,ejc->eic', frames.astype(jnp.float32), message.astype(jnp.float32)).astype(jnp.bfloat16)
    incidence = ((target[None, :] == jnp.arange(atom_count, dtype=jnp.int32)[:, None]) & (valid[None, :] > 0)).astype(jnp.bfloat16)
    summed = jnp.dot(incidence, unrotated.reshape(edge_count, -1), preferred_element_type=jnp.float32)
    return feats32 + summed.reshape(atom_count, components, channels) * (atom_count / edge_count)

def reference(atom_feats, cotangent, frames, radial, edge_source, edge_target, edge_valid, atom_types, dataset, type_table, dataset_table, router_weight, experts):
    count = N_SHARD * N_REPLICA
    comps = atom_feats.shape[1]
    feats_sys = atom_feats.reshape(count, A_DEV, comps, C)
    cot_sys = cotangent.reshape(count, A_DEV, comps, C)
    frames_sys = jnp.moveaxis(frames.reshape(comps, comps, count, E_DEV), 2, 0)
    radial_sys = radial.reshape(count, E_DEV, C)
    source_sys = edge_source.reshape(count, E_DEV)
    target_sys = edge_target.reshape(count, E_DEV)
    valid_sys = edge_valid.reshape(count, E_DEV)
    types_sys = atom_types.reshape(count, A_DEV)
    data_sys = dataset.reshape(count, 1)
    experts32 = experts.astype(jnp.float32)

    def one_system(total, inputs):
        feats, cot, frame, rad, source, target, valid, types, data_one = inputs
        mixture = system_mix(types, data_one, type_table, dataset_table, router_weight)
        merged = jnp.einsum('k,krc->rc', mixture, experts32, precision=lax.Precision.HIGHEST).astype(jnp.bfloat16)
        merged32 = lax.optimization_barrier(merged).astype(jnp.float32)

        def local(feats32, weight32):
            return edge_layer(feats32, weight32, frame, rad, source, target, valid)
        result, pullback = jax.vjp(local, feats.astype(jnp.float32), merged32)
        grad_feats, weight_grad = pullback(cot.astype(jnp.float32))
        partial_value = lax.optimization_barrier((mixture[:, None, None] * weight_grad[None]).astype(jnp.bfloat16))
        return (total + partial_value.astype(jnp.float32), (result.astype(jnp.bfloat16), grad_feats))
    start = jnp.zeros(experts.shape, jnp.float32)
    total, (updated, grads) = lax.scan(one_system, start, (feats_sys, cot_sys, frames_sys, radial_sys, source_sys, target_sys, valid_sys, types_sys, data_sys))
    return (updated.reshape(atom_feats.shape), grads.reshape(atom_feats.shape), total)
```

```python
import functools
import math

import jax
import jax.numpy as jnp
from jax import lax
from jax.experimental import pallas as pl
from jax.experimental.pallas import tpu as pltpu
from jax.sharding import PartitionSpec as P

MESH = pl.DeviceIdType.MESH
VMEM = pltpu.VMEM
F32 = jnp.float32
BF16 = jnp.bfloat16
ROWS = 16
NN = (((1,), (0,)), ((), ()))
NT = (((1,), (1,)), ((), ()))
TN = (((0,), (0,)), ((), ()))


def dot(a, b, dims=NN):
    return lax.dot_general(a, b, dims, preferred_element_type=F32)


def spread(mix, systems, experts, by_expert):
    mix = mix.astype(BF16)
    shape = (experts * ROWS, mix.shape[1])
    pick = (lax.broadcasted_iota(jnp.int32, shape, 0) // ROWS == lax.broadcasted_iota(jnp.int32, shape, 1)).astype(BF16)
    shape = (systems * ROWS, systems)
    own = (lax.broadcasted_iota(jnp.int32, shape, 0) // ROWS == lax.broadcasted_iota(jnp.int32, shape, 1)).astype(BF16)
    if by_expert:
        wide = dot(dot(pick, mix, NT).astype(BF16), own, NT)
    else:
        wide = dot(dot(own, mix).astype(BF16), pick, NT)
    row = lax.broadcasted_iota(jnp.int32, wide.shape, 0) % ROWS
    col = lax.broadcasted_iota(jnp.int32, wide.shape, 1) % ROWS
    return jnp.where(row == col, wide, 0.0).astype(BF16)


def rotate(frame_scr, first, second, out_fn, transposed, channels):
    comps = first.shape[0]

    def step(t, carry):
        at = pl.ds(pl.multiple_of(t * ROWS, ROWS), ROWS)
        edges = first.shape[2]
        one = [first[j, at, :].astype(F32).reshape(2, ROWS // 2, edges) for j in range(comps)]
        two = [second[j, at, :].astype(F32).reshape(2, ROWS // 2, edges) for j in range(comps)]
        for i in range(comps):
            a = b = None
            for j in range(comps):
                f = frame_scr[(j * comps + i) if transposed else (i * comps + j)][None]
                a = f * one[j] if a is None else a + f * one[j]
                b = f * two[j] if b is None else b + f * two[j]
            out_fn(i, at, a.reshape(ROWS, edges), b.reshape(ROWS, edges))
        return carry

    lax.fori_loop(0, channels // ROWS, step, 0)


def fill_frames(frames, frame_scr):
    comps = frames.shape[0]
    for i in range(comps):
        rows = frames[i].astype(F32)
        for j in range(comps):
            frame_scr[i * comps + j] = jnp.broadcast_to(rows[j : j + 1, :], frame_scr.shape[1:])


def hits(index, atoms):
    return lax.broadcasted_iota(jnp.int32, (atoms, index.shape[1]), 0) == index


def before_kernel(
    feats, cot, frames, radial, source, target, valid, types, dataset, type_table, dataset_table, router,
    mix, weight_grad, rotated, dcomb, spread_scr, gat_scr, dun_scr, frame_scr, rad_scr, router_scr,
):
    atoms, comps, channels = feats.shape
    zero_rows = [d * d + d for d in range(math.isqrt(comps))]
    n_types, n_exp = type_table.shape[0], router.shape[1]
    onehot = (lax.broadcasted_iota(jnp.int32, (n_types, atoms), 0) == types[...]).astype(F32)
    counts = jnp.sum(onehot, axis=1, keepdims=True)
    embed = jnp.sum(counts * type_table[...], axis=0, keepdims=True) / atoms
    n_sets = dataset_table.shape[0]
    pick = (lax.broadcasted_iota(jnp.int32, (n_sets, 1), 0) == dataset[...]).astype(F32)
    embed = embed + jnp.sum(pick * dataset_table[...], axis=0, keepdims=True)
    router_scr[...] = jnp.zeros_like(router_scr)
    router_scr[:, :n_exp] = router[...]
    logits = lax.dot_general(embed, router_scr[...], NN, precision=lax.Precision.HIGHEST, preferred_element_type=F32)
    soft = jnp.maximum(logits, 0.0) + jnp.log1p(jnp.exp(-jnp.abs(logits)))
    soft = jnp.where(lax.broadcasted_iota(jnp.int32, soft.shape, 1) < n_exp, soft, 0.0)
    mix[...] = soft / jnp.sum(soft, axis=1, keepdims=True)

    fill_frames(frames, frame_scr)
    rad_scr[...] = radial[...].astype(F32).T
    src = hits(source[...], atoms).astype(BF16)
    tgt = (hits(target[...], atoms) & (valid[...] > 0)).astype(BF16)
    scale = atoms / source.shape[1]
    spread_scr[...] = feats[...].astype(F32)
    for j in range(comps):
        gat_scr[j] = dot(spread_scr[:, j, :].astype(BF16), src, TN).astype(BF16)
    spread_scr[...] = cot[...].astype(F32) * scale
    for j in range(comps):
        dun_scr[j] = dot(spread_scr[:, j, :].astype(BF16), tgt, TN).astype(BF16)

    def out(i, at, a, b):
        rotated[i, at, :] = a.astype(BF16)
        dcomb[i, at, :] = (b.astype(BF16).astype(F32) * rad_scr[at, :]).astype(BF16)

    rotate(frame_scr, gat_scr, dun_scr, out, False, channels)
    for p, i in enumerate(zero_rows):
        for q, j in enumerate(zero_rows):
            weight_grad[p * channels : (p + 1) * channels, q * channels : (q + 1) * channels] = dot(
                rotated[i], dcomb[j], NT
            ).astype(BF16)


def exchange_kernel(
    group, replicas, mix, weight_grad, experts,
    mix_all, rows_all, merged, mix_group, shares, experts_scr, kron_scr,
    local_sem, mix_send, mix_recv, mixall_send, mixall_recv, wg_send, own_send, rows_recv, merged_send, merged_recv,
):
    z, r = lax.axis_index("shard"), lax.axis_index("replica")
    n_exp, block, width = experts.shape
    peers = [lax.rem(z + o, group) for o in range(group)]
    core = lax.rem(r, 2)
    bits = max(replicas.bit_length() - 1, 1)
    dims = [1 << b for b in range(1, bits)]

    def flip(index, bit):
        return index + bit * (1 - 2 * lax.rem(index // bit, 2))

    order = [jnp.where(core == 0, a, b) for a, b in zip(dims, dims[::-1])]
    sibling = flip(r, 1)

    fetch = pltpu.make_async_copy(experts, experts_scr, local_sem.at[0])
    fetch.start()
    keep = pltpu.make_async_copy(
        weight_grad.at[pl.ds(pl.multiple_of(z * block, ROWS), block)], rows_all.at[r, z], local_sem.at[1]
    )
    keep.start()

    barrier = pltpu.get_barrier_semaphore()
    for p in peers[1:]:
        pl.semaphore_signal(barrier, inc=1, device_id=(p, r), device_id_type=MESH)
    for o in range(1, replicas):
        pl.semaphore_signal(barrier, inc=1, device_id=(z, lax.rem(r + o, replicas)), device_id_type=MESH)
    mix_group[z] = mix[...]
    pl.semaphore_wait(barrier, group - 1 + replicas - 1)

    def remote(src, dst, send, recv, device):
        return pltpu.make_async_remote_copy(
            src_ref=src, dst_ref=dst, send_sem=send, recv_sem=recv, device_id=device, device_id_type=MESH
        )

    mix_copies = [
        remote(mix, mix_group.at[z], mix_send.at[n], mix_recv.at[z], (p, r)) for n, p in enumerate(peers[1:])
    ]
    for copy in mix_copies:
        copy.start()
    wg_copies = [
        remote(
            weight_grad.at[pl.ds(pl.multiple_of(p * block, ROWS), block)],
            rows_all.at[r, z], wg_send.at[n], rows_recv.at[r, z], (p, r),
        )
        for n, p in enumerate(peers[1:])
    ]
    for copy in wg_copies:
        copy.start()

    sent = [0]
    pending = []

    def forward(n, mask):
        who = r
        top = -1
        for k in range(len(dims)):
            if mask >> k & 1:
                who = flip(who, order[k])
                top = k
        slot = rows_all.at[who, peers[n]]
        if mask or n:
            remote(slot, slot, own_send.at[0], rows_recv.at[who, peers[n]], (z, r)).wait_recv()
        goals = [flip(r, order[k]) for k in range(top + 1, len(dims))] + [sibling]
        for goal in goals if replicas > 1 else []:
            copy = remote(slot, slot, own_send.at[sent[0]], rows_recv.at[who, peers[n]], (z, goal))
            copy.start()
            pending.append(copy)
            sent[0] += 1

    keep.wait()
    forward(0, 0)

    for n, p in enumerate(peers[1:]):
        remote(mix, mix_group.at[p], mix_send.at[0], mix_recv.at[p], (z, r)).wait_recv()
    mixall_copies = []
    for o in range(1, replicas):
        copy = remote(
            mix_group, mix_all.at[r], mixall_send.at[o - 1], mixall_recv.at[r], (z, lax.rem(r + o, replicas))
        )
        copy.start()
        mixall_copies.append(copy)
    mix_all[r] = mix_group[...]
    kron_scr[...] = spread(mix_group[...].reshape(group, mix.shape[1]), group, n_exp, False)
    fetch.wait()
    for t in range(block // ROWS):
        at = slice(t * ROWS, (t + 1) * ROWS)
        shares[:, at, :] = (
            dot(kron_scr[...], experts_scr[:, at, :].reshape(n_exp * ROWS, width)).astype(BF16).reshape(group, ROWS, width)
        )
    own_rows = pl.ds(pl.multiple_of(z * block, ROWS), block)
    merged_copies = [
        remote(shares.at[p], merged.at[own_rows], merged_send.at[n], merged_recv.at[z], (p, r))
        for n, p in enumerate(peers[1:])
    ]
    for copy in merged_copies:
        copy.start()
    merged[own_rows, :] = shares[z]

    masks = 1 << len(dims)
    for n in range(1, group):
        forward(n, 0)
        for mask in range(1, masks):
            forward(n - 1, mask)
    for mask in range(1, masks):
        forward(group - 1, mask)
    if replicas > 1:
        for n in range(group):
            for mask in range(masks):
                who = sibling
                for k in range(len(dims)):
                    if mask >> k & 1:
                        who = flip(who, dims[k])
                slot = rows_all.at[who, peers[n]]
                remote(slot, slot, own_send.at[0], rows_recv.at[who, peers[n]], (z, r)).wait_recv()
    for o in range(1, replicas):
        who = lax.rem(r + o, replicas)
        remote(mix_group, mix_all.at[who], mixall_send.at[0], mixall_recv.at[who], (z, r)).wait_recv()
    for p in peers[1:]:
        rows = pl.ds(pl.multiple_of(p * block, ROWS), block)
        remote(shares.at[p], merged.at[rows], merged_send.at[0], merged_recv.at[p], (z, r)).wait_recv()
    for copy in mix_copies + wg_copies + mixall_copies + merged_copies + pending:
        copy.wait_send()


def after_kernel(
    feats, cot, frames, radial, source, target, valid, rotated, dcomb, merged, mix_all, rows_all,
    updated, feats_grad, expert_grad,
    spread_scr, msg_scr, drot_scr, un_scr, dgat_scr, frame_scr, rad_scr, kron_scr, out_scr, out_sem,
):
    atoms, comps, channels = feats.shape
    zero_rows = [d * d + d for d in range(math.isqrt(comps))]
    systems, block, width = rows_all.shape
    n_exp = expert_grad.shape[0]
    piece = min(systems, 32)
    tiles = block // ROWS
    copies = []
    for part in range(systems // piece):
        at = slice(part * piece, (part + 1) * piece)
        kron_scr[part] = spread(mix_all[at].reshape(piece, mix_all.shape[2]), piece, n_exp, True)
    for t in range(tiles):
        if t >= 2:
            copies[t - 2].wait()
        rows = slice(t * ROWS, (t + 1) * ROWS)
        total = None
        for part in range(systems // piece):
            at = slice(part * piece, (part + 1) * piece)
            term = dot(kron_scr[part], rows_all[at, rows, :].reshape(piece * ROWS, width))
            total = term if total is None else total + term
        out_scr[t % 2] = total.reshape(n_exp, ROWS, width)
        copy = pltpu.make_async_copy(out_scr.at[t % 2], expert_grad.at[:, rows, :], out_sem.at[t % 2])
        copy.start()
        copies.append(copy)

    fill_frames(frames, frame_scr)
    rad_scr[...] = radial[...].astype(F32).T
    band = len(zero_rows) * channels
    zero_band = jnp.concatenate([rotated[i] for i in zero_rows], axis=0)
    dmixed = jnp.concatenate([dcomb[i] for i in zero_rows], axis=0)
    mixed = dot(merged[...], zero_band, TN)
    dzero = dot(merged[...], dmixed).astype(BF16)
    rad = rad_scr[...]
    for i in range(comps):
        if i in zero_rows:
            at = slice(zero_rows.index(i) * channels, (zero_rows.index(i) + 1) * channels)
            msg_scr[i] = (mixed[at] * rad).astype(BF16)
            drot_scr[i] = dzero[at]
        else:
            msg_scr[i] = (rotated[i].astype(F32) * rad).astype(BF16)
            drot_scr[i] = dcomb[i]

    def out(i, at, a, b):
        un_scr[i, at, :] = a.astype(BF16)
        dgat_scr[i, at, :] = b.astype(BF16)

    rotate(frame_scr, msg_scr, drot_scr, out, True, channels)
    src = hits(source[...], atoms).astype(BF16)
    tgt = (hits(target[...], atoms) & (valid[...] > 0)).astype(BF16)
    scale = atoms / source.shape[1]
    for i in range(comps):
        spread_scr[:, i, :] = dot(tgt, un_scr[i], NT) * scale
        feats_grad[:, i, :] = dot(src, dgat_scr[i], NT).astype(BF16).astype(F32)
    updated[...] = (feats[...].astype(F32) + spread_scr[...]).astype(BF16)
    feats_grad[...] = feats_grad[...] + cot[...].astype(F32)
    for copy in copies[-2:]:
        copy.wait()


def call(kernel, out_shape, scratch, ins, outs=None, collective=None):
    vmem = pl.BlockSpec(memory_space=VMEM)
    anywhere = pl.BlockSpec(memory_space=pl.ANY)
    extra = {} if collective is None else {"collective_id": collective, "has_side_effects": True}
    return pl.pallas_call(
        kernel,
        out_shape=out_shape,
        in_specs=[anywhere if hbm else vmem for hbm in ins],
        out_specs=[anywhere if hbm else vmem for hbm in (outs or [0] * len(out_shape))],
        scratch_shapes=scratch,
        compiler_params=pltpu.CompilerParams(vmem_limit_bytes=56 << 20, **extra),
    )


def shards(
    atom_feats, cotangent, frames, radial, edge_source, edge_target, edge_valid, atom_types, dataset,
    type_table, dataset_table, router_weight, experts,
):
    group, replicas = lax.axis_size("shard"), lax.axis_size("replica")
    atoms, comps, channels = atom_feats.shape
    edges = edge_source.shape[0]
    n_exp, block, width = experts.shape
    source, target, valid = (a.reshape(1, edges) for a in (edge_source, edge_target, edge_valid))
    shape = jax.ShapeDtypeStruct
    stack = (comps, channels, edges)
    lanes = 128
    frame_scr = VMEM((comps * comps, ROWS // 2, edges), F32)
    rad_scr = VMEM((channels, edges), F32)
    mix, weight_grad, rotated, dcomb = call(
        before_kernel,
        [shape((1, lanes), F32), shape((block * group, width), BF16), shape(stack, BF16), shape(stack, BF16)],
        [
            VMEM((atoms, comps, channels), F32), VMEM(stack, BF16), VMEM(stack, BF16), frame_scr, rad_scr,
            VMEM((router_weight.shape[0], lanes), F32),
        ],
        [0] * 12,
    )(
        atom_feats, cotangent, frames, radial, source, target, valid, atom_types.reshape(1, atoms),
        dataset.reshape(1, 1), type_table, dataset_table, router_weight,
    )
    sem = pltpu.SemaphoreType.DMA
    few = max(group - 1, 1)
    many = max(replicas - 1, 1)
    mix_all, rows_all, merged = call(
        functools.partial(exchange_kernel, group, replicas),
        [
            shape((replicas, group, 1, lanes), F32),
            shape((replicas, group, block, width), BF16),
            shape((block * group, width), BF16),
        ],
        [
            VMEM((group, 1, lanes), F32), VMEM((group, block, width), BF16), VMEM(experts.shape, BF16),
            VMEM((group * ROWS, n_exp * ROWS), BF16),
            sem((2,)), sem((few,)), sem((group,)), sem((many,)), sem((replicas,)), sem((few,)),
            sem((many * group,)), sem((replicas, group)), sem((few,)), sem((group,)),
        ],
        [0, 0, 1],
        collective=0,
    )(mix, weight_grad, experts)
    systems = group * replicas
    piece = min(systems, 32)
    updated, feats_grad, expert_grad = call(
        after_kernel,
        [shape(atom_feats.shape, BF16), shape(atom_feats.shape, F32), shape(experts.shape, F32)],
        [
            VMEM((atoms, comps, channels), F32), VMEM(stack, BF16), VMEM(stack, BF16), VMEM(stack, BF16),
            VMEM(stack, BF16), frame_scr, rad_scr, VMEM((systems // piece, n_exp * ROWS, piece * ROWS), BF16),
            VMEM((2, n_exp, ROWS, width), F32), sem((2,)),
        ],
        [0] * 12,
        [0, 0, 1],
    )(
        atom_feats, cotangent, frames, radial, source, target, valid, rotated, dcomb, merged,
        mix_all.reshape(systems, 1, lanes), rows_all.reshape(systems, block, width),
    )
    return (updated, feats_grad, expert_grad)


def solution(mesh):
    both = ("shard", "replica")
    in_specs = (
        P(both, None, None), P(both, None, None), P(None, None, both), P(both, None),
        P(both), P(both), P(both), P(both), P(both), P(), P(), P(), P(None, "shard", None),
    )
    out_specs = (P(both, None, None), P(both, None, None), P(None, "shard", None))
    return jax.shard_map(shards, mesh=mesh, in_specs=in_specs, out_specs=out_specs, check_vma=False)
```

```python
import functools
import math

import jax
import jax.numpy as jnp
from jax import lax
from jax.experimental import pallas as pl
from jax.experimental.pallas import tpu as pltpu
from jax.sharding import PartitionSpec as P

MESH = pl.DeviceIdType.MESH
VMEM = pltpu.VMEM
F32 = jnp.float32
BF16 = jnp.bfloat16
ROWS = 16
NN = (((1,), (0,)), ((), ()))
NT = (((1,), (1,)), ((), ()))
TN = (((0,), (0,)), ((), ()))


def dot(a, b, dims=NN):
    return lax.dot_general(a, b, dims, preferred_element_type=F32)


def spread(mix, systems, experts, by_expert):
    mix = mix.astype(BF16)
    shape = (experts * ROWS, mix.shape[1])
    pick = (lax.broadcasted_iota(jnp.int32, shape, 0) // ROWS == lax.broadcasted_iota(jnp.int32, shape, 1)).astype(BF16)
    shape = (systems * ROWS, systems)
    own = (lax.broadcasted_iota(jnp.int32, shape, 0) // ROWS == lax.broadcasted_iota(jnp.int32, shape, 1)).astype(BF16)
    if by_expert:
        wide = dot(dot(pick, mix, NT).astype(BF16), own, NT)
    else:
        wide = dot(dot(own, mix).astype(BF16), pick, NT)
    row = lax.broadcasted_iota(jnp.int32, wide.shape, 0) % ROWS
    col = lax.broadcasted_iota(jnp.int32, wide.shape, 1) % ROWS
    return jnp.where(row == col, wide, 0.0).astype(BF16)


def rotate(frame_scr, first, second, out_fn, transposed, channels):
    comps = first.shape[0]

    def step(t, carry):
        at = pl.ds(pl.multiple_of(t * ROWS, ROWS), ROWS)
        edges = first.shape[2]
        one = [first[j, at, :].astype(F32).reshape(2, ROWS // 2, edges) for j in range(comps)]
        two = [second[j, at, :].astype(F32).reshape(2, ROWS // 2, edges) for j in range(comps)]
        for i in range(comps):
            a = b = None
            for j in range(comps):
                f = frame_scr[(j * comps + i) if transposed else (i * comps + j)][None]
                a = f * one[j] if a is None else a + f * one[j]
                b = f * two[j] if b is None else b + f * two[j]
            out_fn(i, at, a.reshape(ROWS, edges), b.reshape(ROWS, edges))
        return carry

    lax.fori_loop(0, channels // ROWS, step, 0)


def fill_frames(frames, frame_scr):
    comps = frames.shape[0]
    for i in range(comps):
        rows = frames[i].astype(F32)
        for j in range(comps):
            frame_scr[i * comps + j] = jnp.broadcast_to(rows[j : j + 1, :], frame_scr.shape[1:])


def hits(index, atoms):
    return lax.broadcasted_iota(jnp.int32, (atoms, index.shape[1]), 0) == index


def before_kernel(
    feats, cot, frames, radial, source, target, valid, types, dataset, type_table, dataset_table, router,
    mix, weight_grad, rotated, dcomb, gat_scr, dun_scr, frame_scr, rad_scr, router_scr,
):
    comps, atoms, channels = feats.shape
    zero_rows = [d * d + d for d in range(math.isqrt(comps))]
    n_types, n_exp = type_table.shape[0], router.shape[0]
    onehot = (lax.broadcasted_iota(jnp.int32, (n_types, atoms), 0) == types[...]).astype(F32)
    counts = jnp.sum(onehot, axis=1, keepdims=True)
    embed = jnp.sum(counts * type_table[...], axis=0, keepdims=True) / atoms
    n_sets = dataset_table.shape[0]
    pick = (lax.broadcasted_iota(jnp.int32, (n_sets, 1), 0) == dataset[...]).astype(F32)
    embed = embed + jnp.sum(pick * dataset_table[...], axis=0, keepdims=True)
    router_scr[...] = jnp.zeros_like(router_scr)
    router_scr[:n_exp, :] = router[...]
    logits = lax.dot_general(embed, router_scr[...], NT, precision=lax.Precision.HIGHEST, preferred_element_type=F32)
    soft = jnp.maximum(logits, 0.0) + jnp.log1p(jnp.exp(-jnp.abs(logits)))
    soft = jnp.where(lax.broadcasted_iota(jnp.int32, soft.shape, 1) < n_exp, soft, 0.0)
    mix[...] = soft / jnp.sum(soft, axis=1, keepdims=True)

    fill_frames(frames, frame_scr)
    rad_scr[...] = radial[...].astype(F32).T
    src = hits(source[...], atoms).astype(BF16)
    tgt = (hits(target[...], atoms) & (valid[...] > 0)).astype(BF16)
    scale = atoms / source.shape[1]
    for j in range(comps):
        gat_scr[j] = dot(feats[j], src, TN).astype(BF16)
        dun_scr[j] = (dot(cot[j], tgt, TN) * scale).astype(BF16)

    def out(i, at, a, b):
        rotated[i, at, :] = a.astype(BF16)
        dcomb[i, at, :] = (b.astype(BF16).astype(F32) * rad_scr[at, :]).astype(BF16)

    rotate(frame_scr, gat_scr, dun_scr, out, False, channels)
    for p, i in enumerate(zero_rows):
        for q, j in enumerate(zero_rows):
            weight_grad[p * channels : (p + 1) * channels, q * channels : (q + 1) * channels] = dot(
                rotated[i], dcomb[j], NT
            ).astype(BF16)


def exchange_kernel(
    group, replicas, mix, weight_grad, experts,
    mix_all, rows_all, merged, mix_group, shares, experts_scr, kron_scr,
    local_sem, mix_send, mix_recv, mixall_send, mixall_recv, wg_send, own_send, rows_recv, merged_send, merged_recv,
):
    z, r = lax.axis_index("shard"), lax.axis_index("replica")
    n_exp, block, width = experts.shape
    offsets = sorted(range(group), key=lambda o: min(o, group - o))
    peers = [lax.rem(z + o, group) for o in offsets]
    owners = [lax.rem(z + group - o, group) for o in offsets]
    parts = 2 if block % (2 * ROWS) == 0 else 1
    depth = block // parts
    core = lax.rem(r, 2)
    bits = max(replicas.bit_length() - 1, 1)
    dims = [1 << b for b in range(1, bits)]

    def flip(index, bit):
        return index + bit * (1 - 2 * lax.rem(index // bit, 2))

    order = [jnp.where(core == 0, a, b) for a, b in zip(dims, dims[::-1])]
    sibling = flip(r, 1)

    fetch = pltpu.make_async_copy(experts, experts_scr, local_sem.at[0])
    fetch.start()
    keep = pltpu.make_async_copy(
        weight_grad.at[pl.ds(pl.multiple_of(z * block, ROWS), block)], rows_all.at[r, z], local_sem.at[1]
    )
    keep.start()

    barrier = pltpu.get_barrier_semaphore()
    for p in peers[1:]:
        pl.semaphore_signal(barrier, inc=1, device_id=(p, r), device_id_type=MESH)
    for o in range(1, replicas):
        pl.semaphore_signal(barrier, inc=1, device_id=(z, lax.rem(r + o, replicas)), device_id_type=MESH)
    mix_group[z] = mix[...]
    pl.semaphore_wait(barrier, group - 1 + replicas - 1)

    def remote(src, dst, send, recv, device):
        return pltpu.make_async_remote_copy(
            src_ref=src, dst_ref=dst, send_sem=send, recv_sem=recv, device_id=device, device_id_type=MESH
        )

    mix_copies = [
        remote(mix, mix_group.at[z], mix_send.at[n], mix_recv.at[z], (p, r)) for n, p in enumerate(peers[1:])
    ]
    for copy in mix_copies:
        copy.start()
    wg_copies = [
        remote(
            weight_grad.at[pl.ds(pl.multiple_of(p * block + q * depth, ROWS), depth)],
            rows_all.at[r, z, pl.ds(q * depth, depth)],
            wg_send.at[n * parts + q], rows_recv.at[r, z * parts + q], (p, r),
        )
        for n, p in enumerate(peers[1:])
        for q in range(parts)
    ]
    for copy in wg_copies:
        copy.start()

    sent = [0]
    pending = []

    def slot_of(who, item):
        owner, q = owners[item // parts], item % parts
        return rows_all.at[who, owner, pl.ds(q * depth, depth)], rows_recv.at[who, owner * parts + q]

    def forward(item, mask):
        who = r
        top = -1
        for k in range(len(dims)):
            if mask >> k & 1:
                who = flip(who, order[k])
                top = k
        slot, arrived = slot_of(who, item)
        if mask or item >= parts:
            remote(slot, slot, own_send.at[0], arrived, (z, r)).wait_recv()
        goals = [flip(r, order[k]) for k in range(top + 1, len(dims))] + [sibling]
        for goal in goals if replicas > 1 else []:
            copy = remote(slot, slot, own_send.at[sent[0]], arrived, (z, goal))
            copy.start()
            pending.append(copy)
            sent[0] += 1

    masks = 1 << len(dims)
    keep.wait()
    for item in range(parts):
        forward(item, 0)

    mixall_copies = []
    merged_copies = []
    own_rows = pl.ds(pl.multiple_of(z * block, ROWS), block)
    tiles = block // ROWS

    def mixtures():
        for p in owners[1:]:
            remote(mix, mix_group.at[p], mix_send.at[0], mix_recv.at[p], (z, r)).wait_recv()
        for o in range(1, replicas):
            copy = remote(
                mix_group, mix_all.at[r], mixall_send.at[o - 1], mixall_recv.at[r], (z, lax.rem(r + o, replicas))
            )
            copy.start()
            mixall_copies.append(copy)
        mix_all[r] = mix_group[...]
        kron_scr[...] = spread(mix_group[...].reshape(group, mix.shape[1]), group, n_exp, False)
        fetch.wait()

    def merge(t):
        at = slice(t * ROWS, (t + 1) * ROWS)
        rows = dot(kron_scr[...], experts_scr[:, at, :].reshape(n_exp * ROWS, width))
        shares[:, at, :] = rows.astype(BF16).reshape(group, ROWS, width)

    def send_merged():
        for n, p in enumerate(peers[1:]):
            merged_copies.append(
                remote(shares.at[p], merged.at[own_rows], merged_send.at[n], merged_recv.at[z], (p, r))
            )
            merged_copies[-1].start()
        merged[own_rows, :] = shares[z]

    todo = [mixtures] + [functools.partial(merge, t) for t in range(tiles)] + [send_merged]
    items = group * parts
    for item in range(parts, items + parts):
        if item < items:
            forward(item, 0)
        for mask in range(1, masks):
            forward(item - parts, mask)
        for job in todo[:3]:
            job()
        todo = todo[3:]
    for job in todo:
        job()
    if replicas > 1:
        for item in range(items):
            for mask in range(masks):
                who = sibling
                for k in range(len(dims)):
                    if mask >> k & 1:
                        who = flip(who, dims[k])
                slot, arrived = slot_of(who, item)
                remote(slot, slot, own_send.at[0], arrived, (z, r)).wait_recv()
    for o in range(1, replicas):
        who = lax.rem(r + o, replicas)
        remote(mix_group, mix_all.at[who], mixall_send.at[0], mixall_recv.at[who], (z, r)).wait_recv()
    for p in peers[1:]:
        rows = pl.ds(pl.multiple_of(p * block, ROWS), block)
        remote(shares.at[p], merged.at[rows], merged_send.at[0], merged_recv.at[p], (z, r)).wait_recv()
    for copy in mix_copies + wg_copies + mixall_copies + merged_copies + pending:
        copy.wait_send()


def after_kernel(
    feats, cot, frames, radial, source, target, valid, rotated, dcomb, merged, mix_all, rows_all,
    updated, feats_grad, expert_grad,
    msg_scr, drot_scr, un_scr, dgat_scr, frame_scr, rad_scr, kron_scr, out_scr, out_sem,
):
    comps, atoms, channels = feats.shape
    zero_rows = [d * d + d for d in range(math.isqrt(comps))]
    systems, block, width = rows_all.shape
    n_exp = expert_grad.shape[0]
    piece = min(systems, 32)
    tiles = block // ROWS
    copies = []
    for part in range(systems // piece):
        at = slice(part * piece, (part + 1) * piece)
        kron_scr[part] = spread(mix_all[at].reshape(piece, mix_all.shape[2]), piece, n_exp, True)
    for t in range(tiles):
        if t >= 2:
            copies[t - 2].wait()
        rows = slice(t * ROWS, (t + 1) * ROWS)
        total = None
        for part in range(systems // piece):
            at = slice(part * piece, (part + 1) * piece)
            term = dot(kron_scr[part], rows_all[at, rows, :].reshape(piece * ROWS, width))
            total = term if total is None else total + term
        out_scr[t % 2] = total.reshape(n_exp, ROWS, width)
        copy = pltpu.make_async_copy(out_scr.at[t % 2], expert_grad.at[:, rows, :], out_sem.at[t % 2])
        copy.start()
        copies.append(copy)

    fill_frames(frames, frame_scr)
    rad_scr[...] = radial[...].astype(F32).T
    band = len(zero_rows) * channels
    zero_band = jnp.concatenate([rotated[i] for i in zero_rows], axis=0)
    dmixed = jnp.concatenate([dcomb[i] for i in zero_rows], axis=0)
    mixed = dot(merged[...], zero_band, TN)
    dzero = dot(merged[...], dmixed).astype(BF16)
    rad = rad_scr[...]
    for i in range(comps):
        if i in zero_rows:
            at = slice(zero_rows.index(i) * channels, (zero_rows.index(i) + 1) * channels)
            msg_scr[i] = (mixed[at] * rad).astype(BF16)
            drot_scr[i] = dzero[at]
        else:
            msg_scr[i] = (rotated[i].astype(F32) * rad).astype(BF16)
            drot_scr[i] = dcomb[i]

    def out(i, at, a, b):
        un_scr[i, at, :] = a.astype(BF16)
        dgat_scr[i, at, :] = b.astype(BF16)

    rotate(frame_scr, msg_scr, drot_scr, out, True, channels)
    src = hits(source[...], atoms).astype(BF16)
    tgt = (hits(target[...], atoms) & (valid[...] > 0)).astype(BF16)
    scale = atoms / source.shape[1]
    for i in range(comps):
        updated[i] = (feats[i].astype(F32) + dot(tgt, un_scr[i], NT) * scale).astype(BF16)
        feats_grad[i] = cot[i].astype(F32) + dot(src, dgat_scr[i], NT).astype(BF16).astype(F32)
    for copy in copies[-2:]:
        copy.wait()


def call(kernel, out_shape, scratch, ins, outs=None, collective=None):
    vmem = pl.BlockSpec(memory_space=VMEM)
    anywhere = pl.BlockSpec(memory_space=pl.ANY)
    extra = {} if collective is None else {"collective_id": collective, "has_side_effects": True}
    return pl.pallas_call(
        kernel,
        out_shape=out_shape,
        in_specs=[anywhere if hbm else vmem for hbm in ins],
        out_specs=[anywhere if hbm else vmem for hbm in (outs or [0] * len(out_shape))],
        scratch_shapes=scratch,
        compiler_params=pltpu.CompilerParams(vmem_limit_bytes=56 << 20, **extra),
    )


def shards(
    atom_feats, cotangent, frames, radial, edge_source, edge_target, edge_valid, atom_types, dataset,
    type_table, dataset_table, router_weight, experts,
):
    group, replicas = lax.axis_size("shard"), lax.axis_size("replica")
    atoms, comps, channels = atom_feats.shape
    edges = edge_source.shape[0]
    n_exp, block, width = experts.shape
    feats, cot = atom_feats.transpose(1, 0, 2), cotangent.transpose(1, 0, 2)
    source, target, valid = (a.reshape(1, edges) for a in (edge_source, edge_target, edge_valid))
    shape = jax.ShapeDtypeStruct
    stack = (comps, channels, edges)
    lanes = 128
    frame_scr = VMEM((comps * comps, ROWS // 2, edges), F32)
    rad_scr = VMEM((channels, edges), F32)
    mix, weight_grad, rotated, dcomb = call(
        before_kernel,
        [shape((1, lanes), F32), shape((block * group, width), BF16), shape(stack, BF16), shape(stack, BF16)],
        [
            VMEM(stack, BF16), VMEM(stack, BF16), frame_scr, rad_scr, VMEM((lanes, router_weight.shape[0]), F32),
        ],
        [0] * 12,
    )(
        feats, cot, frames, radial, source, target, valid, atom_types.reshape(1, atoms),
        dataset.reshape(1, 1), type_table, dataset_table, router_weight.T,
    )
    sem = pltpu.SemaphoreType.DMA
    few = max(group - 1, 1)
    parts = 2 if block % (2 * ROWS) == 0 else 1
    many = max(replicas - 1, 1)
    mix_all, rows_all, merged = call(
        functools.partial(exchange_kernel, group, replicas),
        [
            shape((replicas, group, 1, lanes), F32),
            shape((replicas, group, block, width), BF16),
            shape((block * group, width), BF16),
        ],
        [
            VMEM((group, 1, lanes), F32), VMEM((group, block, width), BF16), VMEM(experts.shape, BF16),
            VMEM((group * ROWS, n_exp * ROWS), BF16),
            sem((2,)), sem((few,)), sem((group,)), sem((many,)), sem((replicas,)), sem((few * parts,)),
            sem((many * group * parts,)), sem((replicas, group * parts)), sem((few,)), sem((group,)),
        ],
        [0, 0, 1],
        collective=0,
    )(mix, weight_grad, experts)
    systems = group * replicas
    piece = min(systems, 32)
    updated, feats_grad, expert_grad = call(
        after_kernel,
        [shape(feats.shape, BF16), shape(feats.shape, F32), shape(experts.shape, F32)],
        [
            VMEM(stack, BF16), VMEM(stack, BF16), VMEM(stack, BF16), VMEM(stack, BF16), frame_scr, rad_scr, VMEM((systems // piece, n_exp * ROWS, piece * ROWS), BF16),
            VMEM((2, n_exp, ROWS, width), F32), sem((2,)),
        ],
        [0] * 12,
        [0, 0, 1],
    )(
        feats, cot, frames, radial, source, target, valid, rotated, dcomb, merged,
        mix_all.reshape(systems, 1, lanes), rows_all.reshape(systems, block, width),
    )
    return (updated.transpose(1, 0, 2), feats_grad.transpose(1, 0, 2), expert_grad)


def solution(mesh):
    both = ("shard", "replica")
    in_specs = (
        P(both, None, None), P(both, None, None), P(None, None, both), P(both, None),
        P(both), P(both), P(both), P(both), P(both), P(), P(), P(), P(None, "shard", None),
    )
    out_specs = (P(both, None, None), P(both, None, None), P(None, "shard", None))
    return jax.shard_map(shards, mesh=mesh, in_specs=in_specs, out_specs=out_specs, check_vma=False)
```
